32 devices in a mesh: dp: 1 (over z), ep: 32 (over y, x, core).
Axes of the slice: x: 4, y: 4, z: 1, core: 2. Of those that a mesh axis runs over, the one named last changes fastest.
The devices are a block of a 4x4x8 slice.
Arguments:
- tokens: bfloat16 [24576, 1024], P(('dp', 'ep'))
- expert_ids: int32 [24576, 8], P(('dp', 'ep'))
- gate_wts: float32 [24576, 8], P(('dp', 'ep'))
- slot_ids: int32 [24576, 8], P(('dp', 'ep'))
- w_gate: bfloat16 [32, 1024, 512], P('ep')
- w_up: bfloat16 [32, 1024, 512], P('ep')
- w_down: bfloat16 [32, 512, 1024], P('ep')
Outputs:
- output: bfloat16 [24576, 1024], P(('dp', 'ep'))
All inputs are finite; a program needn't handle non-finite values.
Results may differ from the reference program's by a relative error of at most 0.001.
Values are sent between devices in bfloat16 or wider.
A program may use at most 768 MiB of HBM per device.

```python
import jax
import jax.numpy as jnp
from jax import lax

GROUP_SIZE = 32
TOK_DEV = 768
D_MODEL = 1024
FF_DIM = 512
EXPERTS = 32
TOP_K = 8

TOKENS = GROUP_SIZE * TOK_DEV
SHARD_CAP = 3 * TOK_DEV * TOP_K // (2 * EXPERTS)
CAPACITY = GROUP_SIZE * SHARD_CAP


def draw_routing(route_key, relabel_key):
    relabel = jax.random.permutation(relabel_key, EXPERTS)
    half_a = TOK_DEV // (2 * EXPERTS)
    hot_rows = 3 * half_a
    split_at = hot_rows * (EXPERTS // 2)
    tok_ids = jnp.arange(TOK_DEV)
    base_ids = jnp.where(tok_ids < split_at, tok_ids // hot_rows, EXPERTS // 2 + (tok_ids - split_at) // half_a)
    choice_off = jnp.arange(TOP_K)
    expert_axis = jnp.arange(EXPERTS)

    def one_shard(shard_num):
        shard_key = jax.random.fold_in(route_key, shard_num)
        perm_key, drop_key = jax.random.split(shard_key)
        tok_order = jax.random.permutation(perm_key, TOK_DEV)
        raw_ids = (base_ids[tok_order][:, None] + choice_off[None, :]) % EXPERTS
        drop_draw = jax.random.randint(drop_key, (TOK_DEV, TOP_K), 0, 8)
        keep_mask = (drop_draw != 0) | (raw_ids == TOP_K - 1)
        onehot = ((raw_ids.reshape(-1)[:, None] == expert_axis[None, :]) & keep_mask.reshape(-1)[:, None]).astype(jnp.int32)
        slot_rank = jnp.sum((jnp.cumsum(onehot, axis=0) - onehot) * onehot, axis=1).reshape(TOK_DEV, TOP_K)
        slot_ids = jnp.where(keep_mask, shard_num * SHARD_CAP + slot_rank, -1)
        return relabel[raw_ids].astype(jnp.int32), slot_ids.astype(jnp.int32)

    expert_ids, slot_ids = lax.map(one_shard, jnp.arange(GROUP_SIZE))
    return expert_ids.reshape(TOKENS, TOP_K), slot_ids.reshape(TOKENS, TOP_K)


def draw_weights(weight_key, shape_in, shape_out):
    def one_expert(expert_num):
        draw = jax.random.normal(jax.random.fold_in(weight_key, expert_num), (shape_in, shape_out), jnp.float32)
        return (draw * shape_in ** -0.5).astype(jnp.bfloat16)
    return lax.map(one_expert, jnp.arange(EXPERTS))


def setup_inputs(seed: int = 0, part: int = 0) -> dict:
    root_key = jax.random.key(seed)
    part_keys = jax.random.split(jax.random.fold_in(root_key, part), 4)
    weight_keys = jax.random.split(jax.random.key(seed + 1), 3)
    tokens = jax.random.normal(part_keys[0], (TOKENS, D_MODEL), jnp.float32).astype(jnp.bfloat16)
    gate_wts = jax.random.uniform(part_keys[1], (TOKENS, TOP_K), jnp.float32, minval=0.25, maxval=1.0) * TOP_K ** -0.5
    expert_ids, slot_ids = draw_routing(part_keys[2], part_keys[3])
    return {'tokens': tokens, 'expert_ids': expert_ids, 'gate_wts': gate_wts, 'slot_ids': slot_ids, 'w_gate': draw_weights(weight_keys[0], D_MODEL, FF_DIM), 'w_up': draw_weights(weight_keys[1], D_MODEL, FF_DIM), 'w_down': draw_weights(weight_keys[2], FF_DIM, D_MODEL)}


def reference(tokens, expert_ids, gate_wts, slot_ids, w_gate, w_up, w_down):
    keep_mask = slot_ids >= 0
    flat_slot = jnp.where(keep_mask, expert_ids * CAPACITY + slot_ids, EXPERTS * CAPACITY).reshape(-1)
    tok_index = jnp.broadcast_to(jnp.arange(TOKENS, dtype=jnp.int32)[:, None], expert_ids.shape).reshape(-1)
    slot_token = jnp.full((EXPERTS * CAPACITY,), TOKENS, jnp.int32).at[flat_slot].set(tok_index, mode='drop')
    slot_gate = jnp.zeros((EXPERTS * CAPACITY,), jnp.float32).at[flat_slot].set(gate_wts.reshape(-1), mode='drop')

    def expert_step(accum, scan_in):
        tok_rows, gate_rows, wg_one, wu_one, wd_one = scan_in
        buffer = jnp.take(tokens, tok_rows, axis=0, mode='fill', fill_value=0)
        h_gate = jnp.dot(buffer, wg_one, preferred_element_type=jnp.float32)
        h_up = jnp.dot(buffer, wu_one, preferred_element_type=jnp.float32)
        hidden = (jax.nn.silu(h_gate) * h_up).astype(jnp.bfloat16)
        expert_out = jnp.dot(hidden, wd_one, preferred_element_type=jnp.float32)
        accum = accum.at[tok_rows].add(expert_out * gate_rows[:, None], mode='drop')
        return accum, None

    accum, _ = lax.scan(expert_step, jnp.zeros((TOKENS, D_MODEL), jnp.float32), (slot_token.reshape(EXPERTS, CAPACITY), slot_gate.reshape(EXPERTS, CAPACITY), w_gate, w_up, w_down))
    return accum.astype(jnp.bfloat16)
```

```python
import functools
import math
import jax
import jax.numpy as jnp
from jax import lax
from jax.experimental import pallas as pl
from jax.experimental.pallas import tpu as pltpu
from jax.sharding import PartitionSpec as P

CORES = 2
MESH_ID = pl.DeviceIdType.MESH
PIECES = 4
GU_TILES = 2
DN_TILES = 2

W_SENDS = ((0, 'w', 0), (0, 'w', 1), (1, 'w', 0), (0, 'w', 2), (1, 'w', 1), (0, 'w', 3),
           (0, 'd', 0), (0, 'd', 2), (1, 'd', 0), (0, 'd', 1), (0, 'd', 3), (1, 'd', 1))
W_ISSUE = ((2, 3), (4,), (5,), (6,), (7,), (), (8, 9), (10,), (), (11,), (), ())


def moe_kernel(side, tok_ref, ids_ref, gates_ref, slots_ref, wg_ref, wu_ref, wd_ref, out_ref,
               x, gt, gcol, wgu, wdn, h, part, recv0,
               load_sem, d2d_send, d2d_recv, wr_send, wr_recv, wl_send, wl_recv,
               tr_send, tr_recv, tl_send, tl_recv, rs_send, rs_recv, credit):
    me = lax.axis_index('ep')
    core = lax.rem(me, CORES)
    xx = lax.rem(me // CORES, side)
    yy = me // (CORES * side)
    wi = yy * (1 - core) + xx * core
    ti = xx * (1 - core) + yy * core

    def dev(w_pos, t_pos):
        y_pos = w_pos * (1 - core) + t_pos * core
        x_pos = t_pos * (1 - core) + w_pos * core
        return {'ep': (y_pos * side + x_pos) * CORES + core}

    def ring(pos, off):
        return lax.rem(pos + off + 2 * side, side)

    w_next, w_prev = dev(ring(wi, 1), ti), dev(ring(wi, -1), ti)
    t_next, t_prev = dev(wi, ring(ti, 1)), dev(wi, ring(ti, -1))
    partner = {'ep': me + 1 - 2 * core}

    rows, width = x.shape[1], x.shape[2]
    half = rows // 2
    ff = h.shape[3]
    fp = ff // PIECES
    dp = width // PIECES
    num_q = h.shape[1]

    loads = {}
    for i in range(PIECES):
        for k, src in enumerate((wg_ref, wu_ref)):
            loads['w', i, k] = pltpu.make_async_copy(
                src.at[0, :, pl.ds(i * fp, fp)], wgu.at[wi, i, core, :, pl.ds(k * fp, fp)], load_sem.at[2 * i + k])
        loads['d', i] = pltpu.make_async_copy(
            wd_ref.at[0, :, pl.ds(i * dp, dp)], wdn.at[wi, i, core], load_sem.at[2 * PIECES + i])
    for c in range(2):
        loads['x', c] = pltpu.make_async_copy(
            tok_ref.at[pl.ds(c * half, half)], x.at[ti, pl.ds(c * half, half)], load_sem.at[3 * PIECES + c])
    for c in range(2):
        loads['x', c].start()
    for i in (0, 2, 1, 3):
        loads['w', i, 0].start()
        loads['w', i, 1].start()
    for i in (0, 2, 1, 3):
        loads['d', i].start()

    barrier = pltpu.get_barrier_semaphore()
    for peer in (w_next, w_prev, t_next, t_prev, partner):
        pl.semaphore_signal(barrier, inc=1, device_id=peer, device_id_type=MESH_ID)
    pl.semaphore_wait(barrier, 5)

    def remote(src, dst, s_sem, r_sem, peer):
        return pltpu.make_async_remote_copy(src_ref=src, dst_ref=dst, send_sem=s_sem, recv_sem=r_sem,
                                            device_id=peer, device_id_type=MESH_ID)

    def w_piece(kind, slot, piece):
        return (wgu if kind == 'w' else wdn).at[slot, piece]

    def w_copy(right, n):
        fwd, kind, piece = W_SENDS[n]
        if right:
            ref = w_piece(kind, ring(wi, -fwd), piece)
            return remote(ref, ref, wr_send.at[n], wr_recv.at[n], w_next)
        ref = w_piece(kind, ring(wi, fwd), piece ^ 2)
        return remote(ref, ref, wl_send.at[n], wl_recv.at[n], w_prev)

    def w_wait(n):
        fwd, kind, piece = W_SENDS[n]
        ref = w_piece(kind, ring(wi, -1 - fwd), piece)
        remote(ref, ref, wr_send.at[n], wr_recv.at[n], w_next).wait_recv()
        ref = w_piece(kind, ring(wi, 1 + fwd), piece ^ 2)
        remote(ref, ref, wl_send.at[n], wl_recv.at[n], w_prev).wait_recv()

    def w_issue(n):
        for pos in W_ISSUE[n]:
            w_copy(True, pos).start()
            w_copy(False, pos).start()

    T_RIGHT = ((0, 'x', 0), (0, 'x', 1), (0, 'g', 0), (1, 'x', 0), (1, 'g', 0))
    T_LEFT = ((0, 'x', 1), (0, 'x', 0), (0, 'g', 0), (1, 'x', 1))

    def t_piece(kind, slot, c):
        return x.at[slot, pl.ds(c * half, half)] if kind == 'x' else gt.at[slot]

    def t_copy(right, n):
        fwd, kind, c = (T_RIGHT if right else T_LEFT)[n]
        if right:
            ref = t_piece(kind, ring(ti, -fwd), c)
            return remote(ref, ref, tr_send.at[n], tr_recv.at[n], t_next)
        ref = t_piece(kind, ring(ti, fwd), c)
        return remote(ref, ref, tl_send.at[n], tl_recv.at[n], t_prev)

    def t_wait(right, n):
        fwd, kind, c = (T_RIGHT if right else T_LEFT)[n]
        if right:
            ref = t_piece(kind, ring(ti, -1 - fwd), c)
            remote(ref, ref, tr_send.at[n], tr_recv.at[n], t_next).wait_recv()
        else:
            ref = t_piece(kind, ring(ti, 1 + fwd), c)
            remote(ref, ref, tl_send.at[n], tl_recv.at[n], t_prev).wait_recv()

    loads['x', 0].wait()
    t_copy(True, 0).start()
    loads['x', 1].wait()
    t_copy(False, 0).start()
    t_copy(True, 1).start()
    t_copy(False, 1).start()

    def d2d(kind, i, incoming):
        n = i + (0 if kind == 'w' else PIECES)
        ref = wgu if kind == 'w' else wdn
        mine = ref.at[wi, i, core]
        dst = ref.at[wi, i, 1 - core] if incoming else ref.at[ti, i, core]
        return remote(mine, dst, d2d_send.at[n], d2d_recv.at[n], partner)

    for i in (0, 2, 1, 3):
        loads['w', i, 0].wait()
        loads['w', i, 1].wait()
        d2d('w', i, False).start()
    for i in (0, 2, 1, 3):
        loads['d', i].wait()
        d2d('d', i, False).start()
    for n in range(2):
        d2d('w', n, True).wait_recv()
        w_copy(True, n).start()
        d2d('w', n ^ 2, True).wait_recv()
        w_copy(False, n).start()

    lane = lax.broadcasted_iota(jnp.int32, (gt.shape[1], 1), 0)
    l_t, l_w, l_c = lane // (CORES * side), lax.rem(lane // CORES, side), lax.rem(lane, CORES)
    e_y = l_w * (1 - core) + l_t * core
    e_x = l_t * (1 - core) + l_w * core
    expert = (e_y * side + e_x) * CORES + l_c
    dense = jnp.full(gt.shape[1:], jnp.nan, jnp.float32)
    for j in range(ids_ref.shape[0]):
        hit = (ids_ref[j:j + 1, :] == expert) & (slots_ref[j:j + 1, :] >= 0)
        dense = jnp.where(hit, gates_ref[j:j + 1, :], dense)
    gt[ti] = dense

    for i in (0, 2, 1, 3):
        d2d('d', i, True).wait_recv()

    gu_rows = rows // GU_TILES
    dn_rows = rows // DN_TILES

    def gate_up(shard, hs, slot, piece, cc, rt):
        r = pl.ds(pl.multiple_of(rt * gu_rows, gu_rows), gu_rows)
        both = jnp.dot(x[shard, r, :], wgu[slot, piece, cc], preferred_element_type=jnp.float32)
        a, u = both[:, :fp], both[:, fp:]
        hid = (a * jax.nn.sigmoid(a)) * u
        h[hs, slot * CORES + cc, r, pl.ds(pl.multiple_of(piece * fp, fp), fp)] = hid.astype(jnp.bfloat16)

    def near(s):
        return ring(ti, 2 * s - 1)

    def near_own():
        def body(t, carry):
            s, t2 = t // (PIECES * CORES * GU_TILES), lax.rem(t, PIECES * CORES * GU_TILES)
            piece, t3 = t2 // (CORES * GU_TILES), lax.rem(t2, CORES * GU_TILES)
            gate_up(near(s), s, wi, piece, t3 // GU_TILES, lax.rem(t3, GU_TILES))
            return carry
        lax.fori_loop(0, 2 * PIECES * CORES * GU_TILES, body, 0)

    def arrived(n, d):
        fwd, _, piece = W_SENDS[n]
        return ring(wi, (2 * d - 1) * (1 + fwd)), piece + d * ((piece ^ 2) - piece)

    def near_arrived(n):
        def body(t, carry):
            d, t2 = t // (2 * CORES * GU_TILES), lax.rem(t, 2 * CORES * GU_TILES)
            s, t3 = t2 // (CORES * GU_TILES), lax.rem(t2, CORES * GU_TILES)
            slot, piece = arrived(n, d)
            gate_up(near(s), s, slot, piece, t3 // GU_TILES, lax.rem(t3, GU_TILES))
            return carry
        lax.fori_loop(0, 4 * CORES * GU_TILES, body, 0)

    def whole(shard, hs, first, last):
        per = PIECES * CORES * GU_TILES
        def body(t, carry):
            s, t2 = t // per, lax.rem(t, per)
            piece, t3 = t2 // (CORES * GU_TILES), lax.rem(t2, CORES * GU_TILES)
            gate_up(shard, hs, ring(wi, s), piece, t3 // GU_TILES, lax.rem(t3, GU_TILES))
            return carry
        lax.fori_loop(first * per, last * per, body, 0)

    def far_arrived(n):
        def body(t, carry):
            d, t3 = t // (CORES * GU_TILES), lax.rem(t, CORES * GU_TILES)
            slot, piece = arrived(n, d)
            gate_up(ring(ti, 2), 2, slot, piece, t3 // GU_TILES, lax.rem(t3, GU_TILES))
            return carry
        lax.fori_loop(0, 2 * CORES * GU_TILES, body, 0)

    def gates_to_columns():
        base = pl.ds(pl.multiple_of(ti * num_q, num_q), num_q)
        for s in range(side):
            gcol[s] = jnp.transpose(gt[s, base, :])

    def down(shard, hs, chunk, r, start):
        acc = start
        for q in range(num_q):
            o = jnp.dot(h[hs, q, r, :], wdn[q // CORES, chunk, q % CORES], preferred_element_type=jnp.float32)
            g = jnp.broadcast_to(gcol[shard, r, q:q + 1], o.shape)
            term = jnp.where(g == g, g * o, 0.0)
            acc = term if acc is None else acc + term
        return acc

    def near_down(base, flip):
        def body(t, carry):
            s, rt = t // DN_TILES, lax.rem(t, DN_TILES)
            r = pl.ds(pl.multiple_of(rt * dn_rows, dn_rows), dn_rows)
            shard = s if not flip else 1 - s
            chunk = base + 2 * s
            part[shard, chunk, r, :] = down(near(shard), shard, chunk, r, None)
            return carry
        lax.fori_loop(0, 2 * DN_TILES, body, 0)

    def rs_copy(step, j):
        right = j < 2
        sent = part.at[0, j] if right else part.at[1, j]
        kept = part.at[1, j] if right else part.at[0, j]
        src, dst = ((sent, recv0.at[j]), (recv0.at[j], sent), (sent, kept))[step]
        return remote(src, dst, rs_send.at[step, j], rs_recv.at[step, j], t_next if right else t_prev)

    def give_credit(step, j):
        pl.semaphore_signal(credit.at[step, j], inc=1, device_id=t_prev if j < 2 else t_next, device_id_type=MESH_ID)

    t_wait(True, 0)
    t_wait(False, 0)
    t_copy(True, 2).start()
    t_copy(False, 2).start()
    t_copy(True, 3).start()
    t_copy(False, 3).start()
    w_wait(0)
    w_issue(0)
    t_wait(True, 1)
    t_wait(False, 1)
    near_own()
    w_wait(1)
    w_issue(1)
    near_arrived(0)
    near_arrived(1)
    t_wait(True, 2)
    t_wait(False, 2)
    t_copy(True, 4).start()
    w_wait(2)
    w_issue(2)
    near_arrived(2)
    w_wait(3)
    w_issue(3)
    near_arrived(3)
    t_wait(True, 3)
    t_wait(False, 3)
    t_wait(True, 4)
    gates_to_columns()
    whole(ring(ti, 2), 2, 0, 1)
    w_wait(4)
    w_issue(4)
    near_arrived(4)
    far_arrived(0)
    far_arrived(1)
    w_wait(5)
    w_issue(5)
    near_arrived(5)
    far_arrived(2)
    far_arrived(3)
    w_wait(6)
    w_issue(6)
    far_arrived(4)
    w_wait(7)
    w_issue(7)
    far_arrived(5)
    w_wait(8)
    w_issue(8)
    near_down(0, False)
    rs_copy(0, 0).start()
    rs_copy(0, 2).start()
    w_wait(9)
    w_issue(9)
    near_down(0, True)
    w_wait(10)
    w_wait(11)
    near_down(1, False)
    rs_copy(0, 1).start()
    rs_copy(0, 3).start()
    near_down(1, True)

    far = ring(ti, 2)

    def turn_far(j):
        for k in (j, j + 2):
            rs_copy(0, k).wait_send()
            give_credit(0, k)
        for k in (j, j + 2):
            rs_copy(0, k).wait_recv()

        def body(t, carry):
            chunk, rt = j + 2 * (t // DN_TILES), lax.rem(t, DN_TILES)
            r = pl.ds(pl.multiple_of(rt * dn_rows, dn_rows), dn_rows)
            recv0[chunk, r, :] = down(far, 2, chunk, r, recv0[chunk, r, :])
            return carry
        lax.fori_loop(0, 2 * DN_TILES, body, 0)
        for k in (j, j + 2):
            pl.semaphore_wait(credit.at[0, k], 1)
            rs_copy(1, k).start()

    def turn_near(j):
        for k in (j, j + 2):
            rs_copy(1, k).wait_recv()
        part[0, j] = part[0, j] + part[1, j]
        part[1, j + 2] = part[1, j + 2] + part[0, j + 2]
        for k in (j, j + 2):
            give_credit(1, k)
        for k in (j, j + 2):
            pl.semaphore_wait(credit.at[1, k], 1)
            rs_copy(2, k).start()

    turn_far(0)
    turn_far(1)
    whole(ti, 0, 0, side // 2)
    turn_near(0)
    whole(ti, 0, side // 2, side)
    turn_near(1)
    for j in (0, 2, 1, 3):
        rs_copy(1, j).wait_send()

    def own_body(t, carry):
        chunk, rt = t // DN_TILES, lax.rem(t, DN_TILES)
        r = pl.ds(pl.multiple_of(rt * dn_rows, dn_rows), dn_rows)
        recv0[chunk, r, :] = down(ti, 0, chunk, r, None)
        return carry
    lax.fori_loop(0, PIECES * DN_TILES, own_body, 0)

    for j in (0, 2, 1, 3):
        rs_copy(2, j).wait_recv()
        kept = part[1, j] if j < 2 else part[0, j]
        out_ref[:, j * dp:(j + 1) * dp] = (recv0[j] + kept).astype(out_ref.dtype)

    for j in range(PIECES):
        rs_copy(2, j).wait_send()
    for n in range(len(W_SENDS)):
        w_copy(True, n).wait_send()
        w_copy(False, n).wait_send()
    for n in range(len(T_RIGHT)):
        t_copy(True, n).wait_send()
    for n in range(len(T_LEFT)):
        t_copy(False, n).wait_send()
    for i in range(PIECES):
        d2d('w', i, False).wait_send()
        d2d('d', i, False).wait_send()


def solution(mesh):
    group = mesh.shape['ep']
    side = math.isqrt(group // CORES)
    row_spec = P(('dp', 'ep'), None)
    expert_spec = P('ep', None, None)

    def per_device(tokens, expert_ids, gate_wts, slot_ids, w_gate, w_up, w_down):
        rows, width = tokens.shape
        ff = w_gate.shape[2]
        num_q = CORES * side
        fp, dp = ff // PIECES, width // PIECES
        dma = pltpu.SemaphoreType.DMA
        hbm = pl.BlockSpec(memory_space=pl.ANY)
        vmem = pl.BlockSpec(memory_space=pltpu.VMEM)
        n_w = len(W_SENDS)
        return pl.pallas_call(
            functools.partial(moe_kernel, side),
            out_shape=jax.ShapeDtypeStruct((rows, width), jnp.bfloat16),
            in_specs=[hbm, vmem, vmem, vmem, hbm, hbm, hbm],
            out_specs=vmem,
            scratch_shapes=[
                pltpu.VMEM((side, rows, width), jnp.bfloat16),
                pltpu.VMEM((side, group, rows), jnp.float32),
                pltpu.VMEM((side, rows, num_q), jnp.float32),
                pltpu.VMEM((side, PIECES, CORES, width, 2 * fp), jnp.bfloat16),
                pltpu.VMEM((side, PIECES, CORES, ff, dp), jnp.bfloat16),
                pltpu.VMEM((3, num_q, rows, ff), jnp.bfloat16),
                pltpu.VMEM((2, PIECES, rows, dp), jnp.float32),
                pltpu.VMEM((PIECES, rows, dp), jnp.float32),
                dma((3 * PIECES + 2,)), dma((2 * PIECES,)), dma((2 * PIECES,)),
                dma((n_w,)), dma((n_w,)), dma((n_w,)), dma((n_w,)),
                dma((5,)), dma((5,)), dma((4,)), dma((4,)),
                dma((3, PIECES)), dma((3, PIECES)),
                pltpu.SemaphoreType.REGULAR((2, PIECES)),
            ],
            compiler_params=pltpu.CompilerParams(collective_id=0, has_side_effects=True, vmem_limit_bytes=67043328),
        )(tokens, expert_ids.T, gate_wts.T, slot_ids.T, w_gate, w_up, w_down)

    return jax.shard_map(per_device, mesh=mesh, in_specs=(row_spec, row_spec, row_spec, row_spec, expert_spec, expert_spec, expert_spec), out_specs=row_spec, check_vma=False)
```

```python
import functools
import math
import jax
import jax.numpy as jnp
from jax import lax
from jax.experimental import pallas as pl
from jax.experimental.pallas import tpu as pltpu
from jax.sharding import PartitionSpec as P

CORES = 2
MESH_ID = pl.DeviceIdType.MESH
PIECES = 4
HALVES = 2

W_SENDS = ((0, 'w', 0), (0, 'w', 1), (1, 'w', 0), (0, 'w', 2), (1, 'w', 1), (0, 'w', 3),
           (0, 'd', 0), (0, 'd', 2), (1, 'd', 0), (0, 'd', 1), (0, 'd', 3), (1, 'd', 1))
W_ISSUE = ((2, 3), (4,), (5,), (6,), (7,), (), (8, 9), (10,), (), (11,), (), ())


def moe_kernel(side, tok_ref, ids_ref, gates_ref, slots_ref, wg_ref, wu_ref, wd_ref, out_ref,
               x, gown, gt, gfwd, gcol, wgu, wdn, h, part, recv0,
               load_sem, d2d_send, d2d_recv, wr_send, wr_recv, wl_send, wl_recv,
               tr_send, tr_recv, tl_send, tl_recv, rs_send, rs_recv, credit):
    me = lax.axis_index('ep')
    core = lax.rem(me, CORES)
    xx = lax.rem(me // CORES, side)
    yy = me // (CORES * side)
    wi = yy * (1 - core) + xx * core
    ti = xx * (1 - core) + yy * core

    def dev(w_pos, t_pos):
        y_pos = w_pos * (1 - core) + t_pos * core
        x_pos = t_pos * (1 - core) + w_pos * core
        return {'ep': (y_pos * side + x_pos) * CORES + core}

    def ring(pos, off):
        return lax.rem(pos + off + 2 * side, side)

    w_next, w_prev = dev(ring(wi, 1), ti), dev(ring(wi, -1), ti)
    t_next, t_prev = dev(wi, ring(ti, 1)), dev(wi, ring(ti, -1))
    partner = {'ep': me + 1 - 2 * core}

    rows, width = x.shape[1], x.shape[2]
    half = rows // 2
    ff = h.shape[2]
    fp = ff // PIECES
    dp = width // PIECES
    num_q = CORES * side

    loads = {}
    for i in range(PIECES):
        for k, src in enumerate((wg_ref, wu_ref)):
            loads['w', i, k] = pltpu.make_async_copy(
                src.at[0, :, pl.ds(i * fp, fp)], wgu.at[wi, i, core, :, pl.ds(k * fp, fp)], load_sem.at[2 * i + k])
        loads['d', i] = pltpu.make_async_copy(
            wd_ref.at[0, :, pl.ds(i * dp, dp)], wdn.at[wi, i, core], load_sem.at[2 * PIECES + i])
    for c in range(2):
        loads['x', c] = pltpu.make_async_copy(
            tok_ref.at[pl.ds(c * half, half)], x.at[ti, pl.ds(c * half, half)], load_sem.at[3 * PIECES + c])
    for c in range(2):
        loads['x', c].start()
    for i in (0, 2, 1, 3):
        loads['w', i, 0].start()
        loads['w', i, 1].start()
    for i in (0, 2, 1, 3):
        loads['d', i].start()

    barrier = pltpu.get_barrier_semaphore()
    for peer in (w_next, w_prev, t_next, t_prev, partner):
        pl.semaphore_signal(barrier, inc=1, device_id=peer, device_id_type=MESH_ID)
    pl.semaphore_wait(barrier, 5)

    def remote(src, dst, s_sem, r_sem, peer):
        return pltpu.make_async_remote_copy(src_ref=src, dst_ref=dst, send_sem=s_sem, recv_sem=r_sem,
                                            device_id=peer, device_id_type=MESH_ID)

    def w_piece(kind, slot, piece):
        return (wgu if kind == 'w' else wdn).at[slot, piece]

    def w_copy(right, n):
        fwd, kind, piece = W_SENDS[n]
        if right:
            ref = w_piece(kind, ring(wi, -fwd), piece)
            return remote(ref, ref, wr_send.at[n], wr_recv.at[n], w_next)
        ref = w_piece(kind, ring(wi, fwd), piece ^ 2)
        return remote(ref, ref, wl_send.at[n], wl_recv.at[n], w_prev)

    def w_wait(n):
        fwd, kind, piece = W_SENDS[n]
        ref = w_piece(kind, ring(wi, -1 - fwd), piece)
        remote(ref, ref, wr_send.at[n], wr_recv.at[n], w_next).wait_recv()
        ref = w_piece(kind, ring(wi, 1 + fwd), piece ^ 2)
        remote(ref, ref, wl_send.at[n], wl_recv.at[n], w_prev).wait_recv()

    def w_issue(n):
        for pos in W_ISSUE[n]:
            w_copy(True, pos).start()
            w_copy(False, pos).start()

    def gate_rows(off):
        return gown.at[pl.ds(off * num_q, num_q)]

    def t_refs(right, n, me_t):
        if n in (0, 1):
            ref = x.at[me_t, pl.ds((n if right else 1 - n) * half, half)]
            return ref, ref
        if not right:
            ref = x.at[ring(me_t, 1), pl.ds(half, half)]
            return (gate_rows(side - 1), gt.at[me_t]) if n == 2 else (ref, ref)
        ref = x.at[ring(me_t, -1), pl.ds(0, half)]
        return ((gate_rows(1), gt.at[me_t]), (gate_rows(2), gfwd), (ref, ref), (gfwd, gt.at[ring(me_t, -1)]))[n - 2]

    def t_copy(right, n):
        src, dst = t_refs(right, n, ti)
        if right:
            return remote(src, dst, tr_send.at[n], tr_recv.at[n], t_next)
        return remote(src, dst, tl_send.at[n], tl_recv.at[n], t_prev)

    def t_wait(right, n):
        _, dst = t_refs(right, n, ring(ti, -1 if right else 1))
        if right:
            remote(dst, dst, tr_send.at[n], tr_recv.at[n], t_next).wait_recv()
        else:
            remote(dst, dst, tl_send.at[n], tl_recv.at[n], t_prev).wait_recv()

    loads['x', 0].wait()
    t_copy(True, 0).start()
    loads['x', 1].wait()
    t_copy(False, 0).start()
    t_copy(True, 1).start()
    t_copy(False, 1).start()

    def d2d(kind, i, incoming):
        n = i + (0 if kind == 'w' else PIECES)
        ref = wgu if kind == 'w' else wdn
        mine = ref.at[wi, i, core]
        dst = ref.at[wi, i, 1 - core] if incoming else ref.at[ti, i, core]
        return remote(mine, dst, d2d_send.at[n], d2d_recv.at[n], partner)

    for i in (0, 2, 1, 3):
        loads['w', i, 0].wait()
        loads['w', i, 1].wait()
        d2d('w', i, False).start()
    for i in (0, 2, 1, 3):
        loads['d', i].wait()
        d2d('d', i, False).start()
    for n in range(2):
        d2d('w', n, True).wait_recv()
        w_copy(True, n).start()
        d2d('w', n ^ 2, True).wait_recv()
        w_copy(False, n).start()

    line = lax.broadcasted_iota(jnp.int32, (gown.shape[0], 1), 0)
    l_t, l_w, l_c = lax.rem(line // num_q + ti, side), lax.rem(line // CORES + wi, side), lax.rem(line, CORES)
    e_y = l_w * (1 - core) + l_t * core
    e_x = l_t * (1 - core) + l_w * core
    expert = (e_y * side + e_x) * CORES + l_c
    dense = jnp.full(gown.shape, jnp.nan, jnp.float32)
    for j in range(ids_ref.shape[0]):
        hit = (ids_ref[j:j + 1, :] == expert) & (slots_ref[j:j + 1, :] >= 0)
        dense = jnp.where(hit, gates_ref[j:j + 1, :], dense)
    gown[...] = dense
    gt[ti] = dense[:num_q]

    for i in (0, 2, 1, 3):
        d2d('d', i, True).wait_recv()

    hr = rows // HALVES

    def half_rows(rt):
        return pl.ds(rt * hr, hr)

    def gate_up(shard, base, k, piece):
        slot = ring(wi, k)
        for cc in range(CORES):
            both = jnp.dot(x[shard], wgu[slot, piece, cc], preferred_element_type=jnp.float32)
            a, u = both[:, :fp], both[:, fp:]
            hid = (a / (1.0 + jnp.exp(-a))) * u
            h[base + k * CORES + cc, :, pl.ds(pl.multiple_of(piece * fp, fp), fp)] = hid.astype(jnp.bfloat16)

    FAR = 2 * num_q
    OWN = (3 * num_q, 0)

    def near(s):
        return ring(ti, 2 * s - 1)

    def arrived(n, d):
        fwd, _, piece = W_SENDS[n]
        return side - 1 - fwd + d * (2 + 2 * fwd - side), piece + d * ((piece ^ 2) - piece)

    def near_own():
        def body(t, carry):
            s = lax.rem(t, 2)
            gate_up(near(s), s * num_q, 0, t // 2)
            return carry
        lax.fori_loop(0, 2 * PIECES, body, 0)

    def near_arrived(n):
        def body(t, carry):
            k, piece = arrived(n, t // 2)
            s = lax.rem(t, 2)
            gate_up(near(s), s * num_q, k, piece)
            return carry
        lax.fori_loop(0, 4, body, 0)

    def far_arrived(n):
        def body(t, carry):
            k, piece = arrived(n, t)
            gate_up(far, FAR, k, piece)
            return carry
        lax.fori_loop(0, 2, body, 0)

    def all_pieces(shard, base, first, last):
        def body(t, carry):
            gate_up(shard, base, t // PIECES, lax.rem(t, PIECES))
            return carry
        lax.fori_loop(first * PIECES, last * PIECES, body, 0)

    def gates_to_columns():
        for s, other in ((0, far), (1, ti)):
            gcol[s] = jnp.transpose(jnp.concatenate([gt[near(s)], gt[other]], axis=0))

    far = ring(ti, 2)

    def down(gates, bases, chunk, r, start):
        g_at, g_off = gates
        acc = start
        for q in range(num_q):
            k, cc = q // CORES, q % CORES
            base = bases[k // (side // 2)]
            o = jnp.dot(h[base + q, r, :], wdn[ring(wi, k), chunk, cc], preferred_element_type=jnp.float32)
            g = jnp.broadcast_to(gcol[g_at, r, g_off + q:g_off + q + 1], o.shape)
            term = jnp.where(g == g, g * o, 0.0)
            acc = term if acc is None else acc + term
        return acc

    def near_down(base, rt, flip):
        r = half_rows(rt)

        def body(s, carry):
            shard = s if not flip else 1 - s
            chunk = base + 2 * s
            part[shard, chunk, r, :] = down((shard, 0), (shard * num_q,) * 2, chunk, r, None)
            return carry
        lax.fori_loop(0, 2, body, 0)

    def rs_copy(step, j, rt):
        right = j < 2
        r = half_rows(rt)
        sent = part.at[0 if right else 1, j, r]
        kept = part.at[1 if right else 0, j, r]
        held = recv0.at[j, r]
        src, dst = ((sent, held), (held, sent), (sent, kept))[step]
        return remote(src, dst, rs_send.at[step, j, rt], rs_recv.at[step, j, rt], t_next if right else t_prev)

    def give_credit(step, j, rt):
        pl.semaphore_signal(credit.at[step, j, rt], inc=1, device_id=t_prev if j < 2 else t_next, device_id_type=MESH_ID)

    def first_send(j):
        for rt in range(HALVES):
            near_down(j, rt, False)
            rs_copy(0, j, rt).start()
            rs_copy(0, j + 2, rt).start()

    def keep(j):
        for rt in range(HALVES):
            near_down(j, rt, True)

    def turn_far(j, rt):
        r = half_rows(rt)
        for k in (j, j + 2):
            rs_copy(0, k, rt).wait_send()
            give_credit(0, k, rt)
        for k in (j, j + 2):
            rs_copy(0, k, rt).wait_recv()

        def body(t, carry):
            chunk = j + 2 * t
            recv0[chunk, r, :] = down((0, num_q), (FAR,) * 2, chunk, r, recv0[chunk, r, :])
            return carry
        lax.fori_loop(0, 2, body, 0)
        for k in (j, j + 2):
            pl.semaphore_wait(credit.at[0, k, rt], 1)
            rs_copy(1, k, rt).start()

    def turn_near(j, rt):
        r = half_rows(rt)
        for k in (j, j + 2):
            rs_copy(1, k, rt).wait_recv()
            s = k // 2
            part[s, k, r, :] = part[s, k, r, :] + part[1 - s, k, r, :]
            give_credit(1, k, rt)
        for k in (j, j + 2):
            pl.semaphore_wait(credit.at[1, k, rt], 1)
            rs_copy(2, k, rt).start()

    def own_down(j):
        for k in (j, j + 2):
            for rt in range(HALVES):
                rs_copy(1, k, rt).wait_send()

        def body(t, carry):
            chunk = j + 2 * (t // HALVES)
            r = pl.ds(pl.multiple_of(lax.rem(t, HALVES) * hr, hr), hr)
            recv0[chunk, r, :] = down((1, num_q), OWN, chunk, r, None)
            return carry
        lax.fori_loop(0, 2 * HALVES, body, 0)

    def finish(j, rt):
        r = half_rows(rt)
        for k in (j, j + 2):
            rs_copy(2, k, rt).wait_recv()
            out_ref[r, k * dp:(k + 1) * dp] = (recv0[k, r, :] + part[1 - k // 2, k, r, :]).astype(out_ref.dtype)

    half_k = side // 2
    all_pieces(ti, OWN[0], 0, 1)
    t_wait(True, 0)
    t_wait(False, 0)
    t_copy(True, 2).start()
    t_copy(False, 2).start()
    t_copy(True, 3).start()
    t_copy(True, 4).start()
    t_copy(False, 3).start()
    w_wait(0)
    w_issue(0)
    t_wait(True, 1)
    t_wait(False, 1)
    near_own()
    w_wait(1)
    w_issue(1)
    near_arrived(0)
    near_arrived(1)
    t_wait(True, 2)
    t_wait(False, 2)
    t_wait(True, 3)
    t_copy(True, 5).start()
    w_wait(2)
    w_issue(2)
    near_arrived(2)
    w_wait(3)
    w_issue(3)
    near_arrived(3)
    t_wait(True, 4)
    t_wait(False, 3)
    t_wait(True, 5)
    gates_to_columns()
    all_pieces(far, FAR, 0, 1)
    w_wait(4)
    w_issue(4)
    near_arrived(4)
    far_arrived(0)
    far_arrived(1)
    w_wait(5)
    w_issue(5)
    near_arrived(5)
    far_arrived(2)
    far_arrived(3)
    w_wait(6)
    w_issue(6)
    far_arrived(4)
    w_wait(7)
    w_issue(7)
    far_arrived(5)
    w_wait(8)
    w_issue(8)
    first_send(0)
    w_wait(9)
    w_issue(9)
    keep(0)
    all_pieces(ti, OWN[0], 1, half_k)
    turn_far(0, 0)
    turn_far(0, 1)
    w_wait(10)
    w_wait(11)
    first_send(1)
    keep(1)
    turn_near(0, 0)
    turn_near(0, 1)
    turn_far(1, 0)
    turn_far(1, 1)
    all_pieces(ti, OWN[1], half_k, side)
    own_down(0)
    turn_near(1, 0)
    turn_near(1, 1)
    own_down(1)
    for j in range(2):
        for rt in range(HALVES):
            finish(j, rt)

    for j in range(PIECES):
        for rt in range(HALVES):
            rs_copy(2, j, rt).wait_send()
    for n in range(len(W_SENDS)):
        w_copy(True, n).wait_send()
        w_copy(False, n).wait_send()
    for n in range(6):
        t_copy(True, n).wait_send()
    for n in range(4):
        t_copy(False, n).wait_send()
    for i in range(PIECES):
        d2d('w', i, False).wait_send()
        d2d('d', i, False).wait_send()


def solution(mesh):
    group = mesh.shape['ep']
    side = math.isqrt(group // CORES)
    row_spec = P(('dp', 'ep'), None)
    expert_spec = P('ep', None, None)

    def per_device(tokens, expert_ids, gate_wts, slot_ids, w_gate, w_up, w_down):
        rows, width = tokens.shape
        ff = w_gate.shape[2]
        num_q = CORES * side
        fp, dp = ff // PIECES, width // PIECES
        dma = pltpu.SemaphoreType.DMA
        hbm = pl.BlockSpec(memory_space=pl.ANY)
        vmem = pl.BlockSpec(memory_space=pltpu.VMEM)
        n_w = len(W_SENDS)
        return pl.pallas_call(
            functools.partial(moe_kernel, side),
            out_shape=jax.ShapeDtypeStruct((rows, width), jnp.bfloat16),
            in_specs=[hbm, vmem, vmem, vmem, hbm, hbm, hbm],
            out_specs=vmem,
            scratch_shapes=[
                pltpu.VMEM((side, rows, width), jnp.bfloat16),
                pltpu.VMEM((group, rows), jnp.float32),
                pltpu.VMEM((side, num_q, rows), jnp.float32),
                pltpu.VMEM((num_q, rows), jnp.float32),
                pltpu.VMEM((2, rows, 2 * num_q), jnp.float32),
                pltpu.VMEM((side, PIECES, CORES, width, 2 * fp), jnp.bfloat16),
                pltpu.VMEM((side, PIECES, CORES, ff, dp), jnp.bfloat16),
                pltpu.VMEM((3 * num_q + num_q // 2, rows, ff), jnp.bfloat16),
                pltpu.VMEM((2, PIECES, rows, dp), jnp.float32),
                pltpu.VMEM((PIECES, rows, dp), jnp.float32),
                dma((3 * PIECES + 2,)), dma((2 * PIECES,)), dma((2 * PIECES,)),
                dma((n_w,)), dma((n_w,)), dma((n_w,)), dma((n_w,)),
                dma((6,)), dma((6,)), dma((4,)), dma((4,)),
                dma((3, PIECES, HALVES)), dma((3, PIECES, HALVES)),
                pltpu.SemaphoreType.REGULAR((2, PIECES, HALVES)),
            ],
            compiler_params=pltpu.CompilerParams(collective_id=0, has_side_effects=True, vmem_limit_bytes=67043328),
        )(tokens, expert_ids.T, gate_wts.T, slot_ids.T, w_gate, w_up, w_down)

    return jax.shard_map(per_device, mesh=mesh, in_specs=(row_spec, row_spec, row_spec, row_spec, expert_spec, expert_spec, expert_spec), out_specs=row_spec, check_vma=False)
```

```python
import functools
import math
import jax
import jax.numpy as jnp
from jax import lax
from jax.experimental import pallas as pl
from jax.experimental.pallas import tpu as pltpu
from jax.sharding import PartitionSpec as P

CORES = 2
MESH_ID = pl.DeviceIdType.MESH
PIECES = 4
HALVES = 2

W_SENDS = ((0, 'w', 0), (0, 'w', 1), (1, 'w', 0), (0, 'w', 2), (1, 'w', 1), (0, 'w', 3),
           (0, 'd', 0), (0, 'd', 2), (1, 'd', 0), (0, 'd', 1), (0, 'd', 3), (1, 'd', 1))
W_ISSUE = ((2, 3), (4,), (5,), (6,), (7,), (), (8, 9), (10,), (), (11,), (), ())


def moe_kernel(side, tok_ref, ids_ref, gates_ref, slots_ref, wg_ref, wu_ref, wd_ref, out_ref,
               x, gown, gt, gfwd, gcol, wgu, wdn, h, part, recv0,
               load_sem, d2d_send, d2d_recv, wr_send, wr_recv, wl_send, wl_recv,
               tr_send, tr_recv, tl_send, tl_recv, rs_send, rs_recv, credit):
    me = lax.axis_index('ep')
    core = lax.rem(me, CORES)
    xx = lax.rem(me // CORES, side)
    yy = me // (CORES * side)
    wi = yy * (1 - core) + xx * core
    ti = xx * (1 - core) + yy * core

    def dev(w_pos, t_pos):
        y_pos = w_pos * (1 - core) + t_pos * core
        x_pos = t_pos * (1 - core) + w_pos * core
        return {'ep': (y_pos * side + x_pos) * CORES + core}

    def ring(pos, off):
        return lax.rem(pos + off + 2 * side, side)

    w_next, w_prev = dev(ring(wi, 1), ti), dev(ring(wi, -1), ti)
    t_next, t_prev = dev(wi, ring(ti, 1)), dev(wi, ring(ti, -1))
    partner = {'ep': me + 1 - 2 * core}

    rows, width = x.shape[1], x.shape[2]
    half = rows // 2
    ff = h.shape[2]
    fp = ff // PIECES
    dp = width // PIECES
    num_q = CORES * side

    loads = {}
    for i in range(PIECES):
        for k, src in enumerate((wg_ref, wu_ref)):
            loads['w', i, k] = pltpu.make_async_copy(
                src.at[0, :, pl.ds(i * fp, fp)], wgu.at[wi, i, core, :, pl.ds(k * fp, fp)], load_sem.at[2 * i + k])
        loads['d', i] = pltpu.make_async_copy(
            wd_ref.at[0, :, pl.ds(i * dp, dp)], wdn.at[wi, i, core], load_sem.at[2 * PIECES + i])
    for c in range(2):
        loads['x', c] = pltpu.make_async_copy(
            tok_ref.at[pl.ds(c * half, half)], x.at[ti, pl.ds(c * half, half)], load_sem.at[3 * PIECES + c])
    for c in range(2):
        loads['x', c].start()
    for i in (0, 2, 1, 3):
        loads['w', i, 0].start()
        loads['w', i, 1].start()
    for i in (0, 2, 1, 3):
        loads['d', i].start()

    barrier = pltpu.get_barrier_semaphore()
    for peer in (w_next, w_prev, t_next, t_prev, partner):
        pl.semaphore_signal(barrier, inc=1, device_id=peer, device_id_type=MESH_ID)
    pl.semaphore_wait(barrier, 5)

    def remote(src, dst, s_sem, r_sem, peer):
        return pltpu.make_async_remote_copy(src_ref=src, dst_ref=dst, send_sem=s_sem, recv_sem=r_sem,
                                            device_id=peer, device_id_type=MESH_ID)

    def w_piece(kind, slot, piece):
        return (wgu if kind == 'w' else wdn).at[slot, piece]

    def w_copy(right, n):
        fwd, kind, piece = W_SENDS[n]
        if right:
            ref = w_piece(kind, ring(wi, -fwd), piece)
            return remote(ref, ref, wr_send.at[n], wr_recv.at[n], w_next)
        ref = w_piece(kind, ring(wi, fwd), piece ^ 2)
        return remote(ref, ref, wl_send.at[n], wl_recv.at[n], w_prev)

    def w_wait(n):
        fwd, kind, piece = W_SENDS[n]
        ref = w_piece(kind, ring(wi, -1 - fwd), piece)
        remote(ref, ref, wr_send.at[n], wr_recv.at[n], w_next).wait_recv()
        ref = w_piece(kind, ring(wi, 1 + fwd), piece ^ 2)
        remote(ref, ref, wl_send.at[n], wl_recv.at[n], w_prev).wait_recv()

    def w_issue(n):
        for pos in W_ISSUE[n]:
            w_copy(True, pos).start()
            w_copy(False, pos).start()

    def gate_rows(off):
        return gown.at[pl.ds(off * num_q, num_q)]

    def t_refs(right, n, me_t):
        if n in (0, 1):
            ref = x.at[me_t, pl.ds((n if right else 1 - n) * half, half)]
            return ref, ref
        if not right:
            ref = x.at[ring(me_t, 1), pl.ds(half, half)]
            return (gate_rows(side - 1), gt.at[me_t]) if n == 2 else (ref, ref)
        ref = x.at[ring(me_t, -1), pl.ds(0, half)]
        return ((gate_rows(1), gt.at[me_t]), (gate_rows(2), gfwd), (ref, ref), (gfwd, gt.at[ring(me_t, -1)]))[n - 2]

    def t_copy(right, n):
        src, dst = t_refs(right, n, ti)
        if right:
            return remote(src, dst, tr_send.at[n], tr_recv.at[n], t_next)
        return remote(src, dst, tl_send.at[n], tl_recv.at[n], t_prev)

    def t_wait(right, n):
        _, dst = t_refs(right, n, ring(ti, -1 if right else 1))
        if right:
            remote(dst, dst, tr_send.at[n], tr_recv.at[n], t_next).wait_recv()
        else:
            remote(dst, dst, tl_send.at[n], tl_recv.at[n], t_prev).wait_recv()

    loads['x', 0].wait()
    t_copy(True, 0).start()
    loads['x', 1].wait()
    t_copy(False, 0).start()
    t_copy(True, 1).start()
    t_copy(False, 1).start()

    def d2d(kind, i, incoming):
        n = i + (0 if kind == 'w' else PIECES)
        ref = wgu if kind == 'w' else wdn
        mine = ref.at[wi, i, core]
        dst = ref.at[wi, i, 1 - core] if incoming else ref.at[ti, i, core]
        return remote(mine, dst, d2d_send.at[n], d2d_recv.at[n], partner)

    for i in (0, 2, 1, 3):
        loads['w', i, 0].wait()
        loads['w', i, 1].wait()
        d2d('w', i, False).start()
    for i in (0, 2, 1, 3):
        loads['d', i].wait()
        d2d('d', i, False).start()
    for n in range(2):
        d2d('w', n, True).wait_recv()
        w_copy(True, n).start()
        d2d('w', n ^ 2, True).wait_recv()
        w_copy(False, n).start()

    line = lax.broadcasted_iota(jnp.int32, (gown.shape[0], 1), 0)
    l_t, l_w, l_c = lax.rem(line // num_q + ti, side), lax.rem(line // CORES + wi, side), lax.rem(line, CORES)
    e_y = l_w * (1 - core) + l_t * core
    e_x = l_t * (1 - core) + l_w * core
    expert = (e_y * side + e_x) * CORES + l_c
    dense = jnp.full(gown.shape, jnp.nan, jnp.float32)
    for j in range(ids_ref.shape[0]):
        hit = (ids_ref[j:j + 1, :] == expert) & (slots_ref[j:j + 1, :] >= 0)
        dense = jnp.where(hit, gates_ref[j:j + 1, :], dense)
    gown[...] = dense
    gt[ti] = dense[:num_q]

    for i in (0, 2, 1, 3):
        d2d('d', i, True).wait_recv()

    hr = rows // HALVES

    def half_rows(rt):
        return pl.ds(rt * hr, hr)

    def gate_up(shard, base, k, piece):
        slot = ring(wi, k)
        for cc in range(CORES):
            both = jnp.dot(x[shard], wgu[slot, piece, cc], preferred_element_type=jnp.float32)
            a, u = both[:, :fp], both[:, fp:]
            hid = (a / (1.0 + jnp.exp(-a))) * u
            h[base + k * CORES + cc, :, pl.ds(pl.multiple_of(piece * fp, fp), fp)] = hid.astype(jnp.bfloat16)

    FAR = 2 * num_q
    OWN = (3 * num_q, 0)

    def near(s):
        return ring(ti, 2 * s - 1)

    def arrived(n, d):
        fwd, _, piece = W_SENDS[n]
        return side - 1 - fwd + d * (2 + 2 * fwd - side), piece + d * ((piece ^ 2) - piece)

    def near_own():
        def body(t, carry):
            s = lax.rem(t, 2)
            gate_up(near(s), s * num_q, 0, t // 2)
            return carry
        lax.fori_loop(0, 2 * PIECES, body, 0)

    def near_arrived(n):
        def body(t, carry):
            k, piece = arrived(n, t // 2)
            s = lax.rem(t, 2)
            gate_up(near(s), s * num_q, k, piece)
            return carry
        lax.fori_loop(0, 4, body, 0)

    def far_arrived(n):
        def body(t, carry):
            k, piece = arrived(n, t)
            gate_up(far, FAR, k, piece)
            return carry
        lax.fori_loop(0, 2, body, 0)

    def all_pieces(shard, base, first, last):
        def body(t, carry):
            gate_up(shard, base, t // PIECES, lax.rem(t, PIECES))
            return carry
        lax.fori_loop(first * PIECES, last * PIECES, body, 0)

    def gates_to_columns():
        for s, other in ((0, far), (1, ti)):
            gcol[s] = jnp.transpose(jnp.concatenate([gt[near(s)], gt[other]], axis=0))

    far = ring(ti, 2)

    def down(gates, bases, chunk, r, start):
        g_at, g_off = gates
        acc = start
        for q in range(num_q):
            k, cc = q // CORES, q % CORES
            base = bases[k // (side // 2)]
            o = jnp.dot(h[base + q, r, :], wdn[ring(wi, k), chunk, cc], preferred_element_type=jnp.float32)
            g = jnp.broadcast_to(gcol[g_at, r, g_off + q:g_off + q + 1], o.shape)
            term = jnp.where(g == g, g * o, 0.0)
            acc = term if acc is None else acc + term
        return acc

    def near_down(base, rt, flip):
        r = half_rows(rt)

        def body(s, carry):
            shard = s if not flip else 1 - s
            chunk = base + 2 * s
            part[shard, chunk, r, :] = down((shard, 0), (shard * num_q,) * 2, chunk, r, None)
            return carry
        lax.fori_loop(0, 2, body, 0)

    def rs_copy(step, j, rt):
        right = j < 2
        r = half_rows(rt)
        sent = part.at[0 if right else 1, j, r]
        kept = part.at[1 if right else 0, j, r]
        held = recv0.at[j, r]
        src, dst = ((sent, held), (held, sent), (sent, kept))[step]
        return remote(src, dst, rs_send.at[step, j, rt], rs_recv.at[step, j, rt], t_next if right else t_prev)

    def give_credit(step, j, rt):
        pl.semaphore_signal(credit.at[step, j, rt], inc=1, device_id=t_prev if j < 2 else t_next, device_id_type=MESH_ID)

    def first_send(j):
        for rt in range(HALVES):
            near_down(j, rt, False)
            rs_copy(0, j, rt).start()
            rs_copy(0, j + 2, rt).start()

    def keep(j):
        for rt in range(HALVES):
            near_down(j, rt, True)

    def turn_far(j, rt):
        r = half_rows(rt)
        for k in (j, j + 2):
            rs_copy(0, k, rt).wait_send()
            give_credit(0, k, rt)
        for k in (j, j + 2):
            rs_copy(0, k, rt).wait_recv()

        def body(t, carry):
            chunk = j + 2 * t
            recv0[chunk, r, :] = down((0, num_q), (FAR,) * 2, chunk, r, recv0[chunk, r, :])
            return carry
        lax.fori_loop(0, 2, body, 0)
        for k in (j, j + 2):
            pl.semaphore_wait(credit.at[0, k, rt], 1)
            rs_copy(1, k, rt).start()

    def turn_near(j, rt):
        r = half_rows(rt)
        for k in (j, j + 2):
            rs_copy(1, k, rt).wait_recv()
            s = k // 2
            part[s, k, r, :] = part[s, k, r, :] + part[1 - s, k, r, :]
            give_credit(1, k, rt)
        for k in (j, j + 2):
            pl.semaphore_wait(credit.at[1, k, rt], 1)
            rs_copy(2, k, rt).start()

    def own_down(j):
        for k in (j, j + 2):
            for rt in range(HALVES):
                rs_copy(1, k, rt).wait_send()

        def body(t, carry):
            chunk = j + 2 * (t // HALVES)
            r = pl.ds(pl.multiple_of(lax.rem(t, HALVES) * hr, hr), hr)
            recv0[chunk, r, :] = down((1, num_q), OWN, chunk, r, None)
            return carry
        lax.fori_loop(0, 2 * HALVES, body, 0)

    def finish(j, rt):
        r = half_rows(rt)
        for k in (j, j + 2):
            rs_copy(2, k, rt).wait_recv()
            out_ref[r, k * dp:(k + 1) * dp] = (recv0[k, r, :] + part[1 - k // 2, k, r, :]).astype(out_ref.dtype)

    half_k = side // 2
    all_pieces(ti, OWN[0], 0, 1)
    t_wait(True, 0)
    t_wait(False, 0)
    t_copy(True, 2).start()
    t_copy(False, 2).start()
    t_copy(True, 3).start()
    t_copy(True, 4).start()
    t_copy(False, 3).start()
    w_wait(0)
    w_issue(0)
    t_wait(True, 1)
    t_wait(False, 1)
    near_own()
    w_wait(1)
    w_issue(1)
    near_arrived(0)
    near_arrived(1)
    t_wait(True, 2)
    t_wait(False, 2)
    t_wait(True, 3)
    t_copy(True, 5).start()
    w_wait(2)
    w_issue(2)
    near_arrived(2)
    w_wait(3)
    w_issue(3)
    near_arrived(3)
    t_wait(True, 4)
    t_wait(False, 3)
    t_wait(True, 5)
    gates_to_columns()
    all_pieces(far, FAR, 0, 1)
    w_wait(4)
    w_issue(4)
    near_arrived(4)
    far_arrived(0)
    far_arrived(1)
    w_wait(5)
    w_issue(5)
    near_arrived(5)
    far_arrived(2)
    far_arrived(3)
    w_wait(6)
    w_issue(6)
    far_arrived(4)
    w_wait(7)
    w_issue(7)
    far_arrived(5)
    w_wait(8)
    w_issue(8)
    first_send(0)
    w_wait(9)
    w_issue(9)
    keep(0)
    all_pieces(ti, OWN[0], 1, half_k)
    turn_far(0, 0)
    turn_far(0, 1)
    w_wait(10)
    w_wait(11)
    first_send(1)
    keep(1)
    turn_near(0, 0)
    turn_near(0, 1)
    turn_far(1, 0)
    turn_far(1, 1)
    all_pieces(ti, OWN[1], half_k, side)
    turn_near(1, 0)
    own_down(0)
    turn_near(1, 1)
    own_down(1)
    for j in range(2):
        for rt in range(HALVES):
            finish(j, rt)

    for j in range(PIECES):
        for rt in range(HALVES):
            rs_copy(2, j, rt).wait_send()
    for n in range(len(W_SENDS)):
        w_copy(True, n).wait_send()
        w_copy(False, n).wait_send()
    for n in range(6):
        t_copy(True, n).wait_send()
    for n in range(4):
        t_copy(False, n).wait_send()
    for i in range(PIECES):
        d2d('w', i, False).wait_send()
        d2d('d', i, False).wait_send()


def place_kernel(src_ref, dst_ref, sem):
    copy = pltpu.make_async_copy(src_ref, dst_ref, sem.at[0])
    copy.start()
    copy.wait()


def solution(mesh):
    group = mesh.shape['ep']
    side = math.isqrt(group // CORES)
    row_spec = P(('dp', 'ep'), None)
    expert_spec = P('ep', None, None)

    def per_device(tokens, expert_ids, gate_wts, slot_ids, w_gate, w_up, w_down):
        rows, width = tokens.shape
        ff = w_gate.shape[2]
        num_q = CORES * side
        fp, dp = ff // PIECES, width // PIECES
        dma = pltpu.SemaphoreType.DMA
        hbm = pl.BlockSpec(memory_space=pl.ANY)
        vmem = pl.BlockSpec(memory_space=pltpu.VMEM)
        n_w = len(W_SENDS)
        result = pl.pallas_call(
            functools.partial(moe_kernel, side),
            out_shape=pltpu.VMEM((rows, width), jnp.bfloat16),
            in_specs=[hbm, vmem, vmem, vmem, hbm, hbm, hbm],
            out_specs=vmem,
            scratch_shapes=[
                pltpu.VMEM((side, rows, width), jnp.bfloat16),
                pltpu.VMEM((group, rows), jnp.float32),
                pltpu.VMEM((side, num_q, rows), jnp.float32),
                pltpu.VMEM((num_q, rows), jnp.float32),
                pltpu.VMEM((2, rows, 2 * num_q), jnp.float32),
                pltpu.VMEM((side, PIECES, CORES, width, 2 * fp), jnp.bfloat16),
                pltpu.VMEM((side, PIECES, CORES, ff, dp), jnp.bfloat16),
                pltpu.VMEM((3 * num_q + num_q // 2, rows, ff), jnp.bfloat16),
                pltpu.VMEM((2, PIECES, rows, dp), jnp.float32),
                pltpu.VMEM((PIECES, rows, dp), jnp.float32),
                dma((3 * PIECES + 2,)), dma((2 * PIECES,)), dma((2 * PIECES,)),
                dma((n_w,)), dma((n_w,)), dma((n_w,)), dma((n_w,)),
                dma((6,)), dma((6,)), dma((4,)), dma((4,)),
                dma((3, PIECES, HALVES)), dma((3, PIECES, HALVES)),
                pltpu.SemaphoreType.REGULAR((2, PIECES, HALVES)),
            ],
            compiler_params=pltpu.CompilerParams(collective_id=0, has_side_effects=True, vmem_limit_bytes=67043328 - rows * width * 2),
        )(tokens, expert_ids.T, gate_wts.T, slot_ids.T, w_gate, w_up, w_down)
        return pl.pallas_call(
            place_kernel,
            out_shape=jax.ShapeDtypeStruct((rows, width), jnp.bfloat16),
            in_specs=[vmem],
            out_specs=hbm,
            scratch_shapes=[dma((1,))],
            compiler_params=pltpu.CompilerParams(vmem_limit_bytes=1 << 20),
        )(result)

    return jax.shard_map(per_device, mesh=mesh, in_specs=(row_spec, row_spec, row_spec, row_spec, expert_spec, expert_spec, expert_spec), out_specs=row_spec, check_vma=False)
```

```python
import functools
import math
import jax
import jax.numpy as jnp
from jax import lax
from jax.experimental import pallas as pl
from jax.experimental.pallas import tpu as pltpu
from jax.sharding import PartitionSpec as P

CORES = 2
MESH_ID = pl.DeviceIdType.MESH
PIECES = 4
HALVES = 2

W_SENDS = ((0, 'w', 0), (0, 'w', 1), (1, 'w', 0), (0, 'w', 2), (1, 'w', 1), (0, 'w', 3),
           (0, 'd', 0), (0, 'd', 2), (1, 'd', 0), (0, 'd', 1), (0, 'd', 3), (1, 'd', 1))
W_ISSUE = ((2, 3), (4,), (5,), (6,), (7,), (), (8, 9), (10,), (), (11,), (), ())


def moe_kernel(side, tok_ref, ids_ref, gates_ref, slots_ref, wg_ref, wu_ref, wd_ref, out_ref,
               x, gown, gt, gfwd, gcol, wgu, wdn, h, part, recv0,
               load_sem, d2d_send, d2d_recv, wr_send, wr_recv, wl_send, wl_recv,
               tr_send, tr_recv, tl_send, tl_recv, rs_send, rs_recv, credit):
    me = lax.axis_index('ep')
    core = lax.rem(me, CORES)
    xx = lax.rem(me // CORES, side)
    yy = me // (CORES * side)
    wi = yy * (1 - core) + xx * core
    ti = xx * (1 - core) + yy * core

    def dev(w_pos, t_pos):
        y_pos = w_pos * (1 - core) + t_pos * core
        x_pos = t_pos * (1 - core) + w_pos * core
        return {'ep': (y_pos * side + x_pos) * CORES + core}

    def ring(pos, off):
        return lax.rem(pos + off + 2 * side, side)

    w_next, w_prev = dev(ring(wi, 1), ti), dev(ring(wi, -1), ti)
    t_next, t_prev = dev(wi, ring(ti, 1)), dev(wi, ring(ti, -1))
    partner = {'ep': me + 1 - 2 * core}

    rows, width = x.shape[1], x.shape[2]
    half = rows // 2
    ff = h.shape[2]
    fp = ff // PIECES
    dp = width // PIECES
    num_q = CORES * side

    loads = {}
    for i in range(PIECES):
        for k, src in enumerate((wg_ref, wu_ref)):
            loads['w', i, k] = pltpu.make_async_copy(
                src.at[0, :, pl.ds(i * fp, fp)], wgu.at[wi, i, core, :, pl.ds(k * fp, fp)], load_sem.at[2 * i + k])
        loads['d', i] = pltpu.make_async_copy(
            wd_ref.at[0, :, pl.ds(i * dp, dp)], wdn.at[wi, i, core], load_sem.at[2 * PIECES + i])
    for c in range(2):
        loads['x', c] = pltpu.make_async_copy(
            tok_ref.at[pl.ds(c * half, half)], x.at[ti, pl.ds(c * half, half)], load_sem.at[3 * PIECES + c])
    for c in range(2):
        loads['x', c].start()
    for i in (0, 2, 1, 3):
        loads['w', i, 0].start()
        loads['w', i, 1].start()
    for i in (0, 2, 1, 3):
        loads['d', i].start()

    barrier = pltpu.get_barrier_semaphore()
    for peer in (w_next, w_prev, t_next, t_prev, partner):
        pl.semaphore_signal(barrier, inc=1, device_id=peer, device_id_type=MESH_ID)
    pl.semaphore_wait(barrier, 5)

    def remote(src, dst, s_sem, r_sem, peer):
        return pltpu.make_async_remote_copy(src_ref=src, dst_ref=dst, send_sem=s_sem, recv_sem=r_sem,
                                            device_id=peer, device_id_type=MESH_ID)

    def w_piece(kind, slot, piece):
        return (wgu if kind == 'w' else wdn).at[slot, piece]

    def w_copy(right, n):
        fwd, kind, piece = W_SENDS[n]
        if right:
            ref = w_piece(kind, ring(wi, -fwd), piece)
            return remote(ref, ref, wr_send.at[n], wr_recv.at[n], w_next)
        ref = w_piece(kind, ring(wi, fwd), piece ^ 2)
        return remote(ref, ref, wl_send.at[n], wl_recv.at[n], w_prev)

    def w_wait(n):
        fwd, kind, piece = W_SENDS[n]
        ref = w_piece(kind, ring(wi, -1 - fwd), piece)
        remote(ref, ref, wr_send.at[n], wr_recv.at[n], w_next).wait_recv()
        ref = w_piece(kind, ring(wi, 1 + fwd), piece ^ 2)
        remote(ref, ref, wl_send.at[n], wl_recv.at[n], w_prev).wait_recv()

    def w_issue(n):
        for pos in W_ISSUE[n]:
            w_copy(True, pos).start()
            w_copy(False, pos).start()

    def gate_rows(off):
        return gown.at[pl.ds(off * num_q, num_q)]

    def t_refs(right, n, me_t):
        if n in (0, 1):
            ref = x.at[me_t, pl.ds((n if right else 1 - n) * half, half)]
            return ref, ref
        if not right:
            ref = x.at[ring(me_t, 1), pl.ds(half, half)]
            return (gate_rows(side - 1), gt.at[me_t]) if n == 2 else (ref, ref)
        ref = x.at[ring(me_t, -1), pl.ds(0, half)]
        return ((gate_rows(1), gt.at[me_t]), (gate_rows(2), gfwd), (ref, ref), (gfwd, gt.at[ring(me_t, -1)]))[n - 2]

    def t_copy(right, n):
        src, dst = t_refs(right, n, ti)
        if right:
            return remote(src, dst, tr_send.at[n], tr_recv.at[n], t_next)
        return remote(src, dst, tl_send.at[n], tl_recv.at[n], t_prev)

    def t_wait(right, n):
        _, dst = t_refs(right, n, ring(ti, -1 if right else 1))
        if right:
            remote(dst, dst, tr_send.at[n], tr_recv.at[n], t_next).wait_recv()
        else:
            remote(dst, dst, tl_send.at[n], tl_recv.at[n], t_prev).wait_recv()

    loads['x', 0].wait()
    t_copy(True, 0).start()
    loads['x', 1].wait()
    t_copy(False, 0).start()
    t_copy(True, 1).start()
    t_copy(False, 1).start()

    def d2d(kind, i, incoming):
        n = i + (0 if kind == 'w' else PIECES)
        ref = wgu if kind == 'w' else wdn
        mine = ref.at[wi, i, core]
        dst = ref.at[wi, i, 1 - core] if incoming else ref.at[ti, i, core]
        return remote(mine, dst, d2d_send.at[n], d2d_recv.at[n], partner)

    for i in (0, 2, 1, 3):
        loads['w', i, 0].wait()
        loads['w', i, 1].wait()
        d2d('w', i, False).start()
    for i in (0, 2, 1, 3):
        loads['d', i].wait()
        d2d('d', i, False).start()
    for n in range(2):
        d2d('w', n, True).wait_recv()
        w_copy(True, n).start()
        d2d('w', n ^ 2, True).wait_recv()
        w_copy(False, n).start()

    line = lax.broadcasted_iota(jnp.int32, (gown.shape[0], 1), 0)
    l_t, l_w, l_c = lax.rem(line // num_q + ti, side), lax.rem(line // CORES + wi, side), lax.rem(line, CORES)
    e_y = l_w * (1 - core) + l_t * core
    e_x = l_t * (1 - core) + l_w * core
    expert = (e_y * side + e_x) * CORES + l_c
    dense = jnp.full(gown.shape, jnp.nan, jnp.float32)
    for j in range(ids_ref.shape[0]):
        hit = (ids_ref[j:j + 1, :] == expert) & (slots_ref[j:j + 1, :] >= 0)
        dense = jnp.where(hit, gates_ref[j:j + 1, :], dense)
    gown[...] = dense
    gt[ti] = dense[:num_q]

    for i in (0, 2, 1, 3):
        d2d('d', i, True).wait_recv()

    hr = rows // HALVES

    def half_rows(rt):
        return pl.ds(rt * hr, hr)

    def gate_up(shard, base, k, piece):
        slot = ring(wi, k)
        for cc in range(CORES):
            both = jnp.dot(x[shard], wgu[slot, piece, cc], preferred_element_type=jnp.float32)
            a, u = both[:, :fp], both[:, fp:]
            hid = (a / (1.0 + jnp.exp(-a))) * u
            h[base + k * CORES + cc, :, pl.ds(pl.multiple_of(piece * fp, fp), fp)] = hid.astype(jnp.bfloat16)

    FAR = 2 * num_q
    OWN = (3 * num_q, 0)

    def near(s):
        return ring(ti, 2 * s - 1)

    def arrived(n, d):
        fwd, _, piece = W_SENDS[n]
        return side - 1 - fwd + d * (2 + 2 * fwd - side), piece + d * ((piece ^ 2) - piece)

    def near_own():
        def body(t, carry):
            s = lax.rem(t, 2)
            gate_up(near(s), s * num_q, 0, t // 2)
            return carry
        lax.fori_loop(0, 2 * PIECES, body, 0)

    def near_arrived(n):
        def body(t, carry):
            k, piece = arrived(n, t // 2)
            s = lax.rem(t, 2)
            gate_up(near(s), s * num_q, k, piece)
            return carry
        lax.fori_loop(0, 4, body, 0)

    def far_arrived(n):
        def body(t, carry):
            k, piece = arrived(n, t)
            gate_up(far, FAR, k, piece)
            return carry
        lax.fori_loop(0, 2, body, 0)

    def all_pieces(shard, base, first, last):
        def body(t, carry):
            gate_up(shard, base, t // PIECES, lax.rem(t, PIECES))
            return carry
        lax.fori_loop(first * PIECES, last * PIECES, body, 0)

    def gates_to_columns():
        for s, other in ((0, far), (1, ti)):
            gcol[s] = jnp.transpose(jnp.concatenate([gt[near(s)], gt[other]], axis=0))

    far = ring(ti, 2)

    ALL_K = tuple(range(side))
    LAST_K = (side // 2,)
    EARLY_K = tuple(k for k in ALL_K if k not in LAST_K)

    def down(gates, bases, chunk, r, start, ks=ALL_K):
        g_at, g_off = gates
        acc = start
        for k in ks:
            for q in range(k * CORES, (k + 1) * CORES):
                h_row = bases[k // (side // 2)] + q
                o = jnp.dot(h[h_row, r, :], wdn[ring(wi, k), chunk, q % CORES], preferred_element_type=jnp.float32)
                g = jnp.broadcast_to(gcol[g_at, r, g_off + q:g_off + q + 1], o.shape)
                term = jnp.where(g == g, g * o, 0.0)
                acc = term if acc is None else acc + term
        return acc

    def near_down(base, rt, flip, ks=ALL_K, more=False):
        r = half_rows(rt)

        def body(s, carry):
            shard = s if not flip else 1 - s
            chunk = base + 2 * s
            start = part[shard, chunk, r, :] if more else None
            part[shard, chunk, r, :] = down((shard, 0), (shard * num_q,) * 2, chunk, r, start, ks)
            return carry
        lax.fori_loop(0, 2, body, 0)

    def rs_copy(step, j, rt):
        right = j < 2
        r = half_rows(rt)
        sent = part.at[0 if right else 1, j, r]
        kept = part.at[1 if right else 0, j, r]
        held = recv0.at[j, r]
        src, dst = ((sent, held), (held, sent), (sent, kept))[step]
        return remote(src, dst, rs_send.at[step, j, rt], rs_recv.at[step, j, rt], t_next if right else t_prev)

    def give_credit(step, j, rt):
        pl.semaphore_signal(credit.at[step, j, rt], inc=1, device_id=t_prev if j < 2 else t_next, device_id_type=MESH_ID)

    def first_part(j):
        for rt in range(HALVES):
            near_down(j, rt, False, EARLY_K)

    def first_send(j):
        for rt in range(HALVES):
            near_down(j, rt, False, LAST_K, True)
            rs_copy(0, j, rt).start()
            rs_copy(0, j + 2, rt).start()

    def keep(j):
        for rt in range(HALVES):
            near_down(j, rt, True)

    def turn_far(j, rt):
        r = half_rows(rt)
        for k in (j, j + 2):
            rs_copy(0, k, rt).wait_send()
            give_credit(0, k, rt)
        for k in (j, j + 2):
            rs_copy(0, k, rt).wait_recv()

        def body(t, carry):
            chunk = j + 2 * t
            recv0[chunk, r, :] = down((0, num_q), (FAR,) * 2, chunk, r, recv0[chunk, r, :])
            return carry
        lax.fori_loop(0, 2, body, 0)
        for k in (j, j + 2):
            pl.semaphore_wait(credit.at[0, k, rt], 1)
            rs_copy(1, k, rt).start()

    def turn_near(j, rt):
        r = half_rows(rt)
        for k in (j, j + 2):
            rs_copy(1, k, rt).wait_recv()
            s = k // 2
            part[s, k, r, :] = part[s, k, r, :] + part[1 - s, k, r, :]
            give_credit(1, k, rt)
        for k in (j, j + 2):
            pl.semaphore_wait(credit.at[1, k, rt], 1)
            rs_copy(2, k, rt).start()

    def own_down(j):
        for k in (j, j + 2):
            for rt in range(HALVES):
                rs_copy(1, k, rt).wait_send()

        def body(t, carry):
            chunk = j + 2 * (t // HALVES)
            r = pl.ds(pl.multiple_of(lax.rem(t, HALVES) * hr, hr), hr)
            recv0[chunk, r, :] = down((1, num_q), OWN, chunk, r, None)
            return carry
        lax.fori_loop(0, 2 * HALVES, body, 0)

    def finish(j, rt):
        r = half_rows(rt)
        for k in (j, j + 2):
            rs_copy(2, k, rt).wait_recv()
            out_ref[r, k * dp:(k + 1) * dp] = (recv0[k, r, :] + part[1 - k // 2, k, r, :]).astype(out_ref.dtype)

    half_k = side // 2
    all_pieces(ti, OWN[0], 0, 1)
    t_wait(True, 0)
    t_wait(False, 0)
    t_copy(True, 2).start()
    t_copy(False, 2).start()
    t_copy(True, 3).start()
    t_copy(True, 4).start()
    t_copy(False, 3).start()
    w_wait(0)
    w_issue(0)
    t_wait(True, 1)
    t_wait(False, 1)
    near_own()
    w_wait(1)
    w_issue(1)
    near_arrived(0)
    near_arrived(1)
    t_wait(True, 2)
    t_wait(False, 2)
    t_wait(True, 3)
    t_copy(True, 5).start()
    w_wait(2)
    w_issue(2)
    near_arrived(2)
    w_wait(3)
    w_issue(3)
    near_arrived(3)
    t_wait(True, 4)
    t_wait(False, 3)
    t_wait(True, 5)
    gates_to_columns()
    all_pieces(far, FAR, 0, 1)
    w_wait(4)
    w_issue(4)
    near_arrived(4)
    far_arrived(0)
    far_arrived(1)
    w_wait(5)
    w_issue(5)
    near_arrived(5)
    far_arrived(2)
    far_arrived(3)
    w_wait(6)
    w_issue(6)
    far_arrived(4)
    w_wait(7)
    w_issue(7)
    first_part(0)
    w_wait(8)
    w_issue(8)
    first_send(0)
    far_arrived(5)
    w_wait(9)
    w_issue(9)
    keep(0)
    all_pieces(ti, OWN[0], 1, half_k)
    turn_far(0, 0)
    turn_far(0, 1)
    w_wait(10)
    first_part(1)
    w_wait(11)
    first_send(1)
    keep(1)
    turn_near(0, 0)
    turn_near(0, 1)
    turn_far(1, 0)
    turn_far(1, 1)
    all_pieces(ti, OWN[1], half_k, side)
    turn_near(1, 0)
    own_down(0)
    turn_near(1, 1)
    own_down(1)
    finish(0, 0)
    finish(0, 1)
    for j in range(PIECES):
        for rt in range(HALVES):
            if j % 2 == 0 or rt == 0:
                rs_copy(2, j, rt).wait_send()
    for n in range(len(W_SENDS)):
        w_copy(True, n).wait_send()
        w_copy(False, n).wait_send()
    for n in range(6):
        t_copy(True, n).wait_send()
    for n in range(4):
        t_copy(False, n).wait_send()
    for i in range(PIECES):
        d2d('w', i, False).wait_send()
        d2d('d', i, False).wait_send()
    finish(1, 0)
    finish(1, 1)
    for j in range(1, PIECES, 2):
        rs_copy(2, j, 1).wait_send()


def place_kernel(src_ref, dst_ref, sem):
    copy = pltpu.make_async_copy(src_ref, dst_ref, sem.at[0])
    copy.start()
    copy.wait()


def solution(mesh):
    group = mesh.shape['ep']
    side = math.isqrt(group // CORES)
    row_spec = P(('dp', 'ep'), None)
    expert_spec = P('ep', None, None)

    def per_device(tokens, expert_ids, gate_wts, slot_ids, w_gate, w_up, w_down):
        rows, width = tokens.shape
        ff = w_gate.shape[2]
        num_q = CORES * side
        fp, dp = ff // PIECES, width // PIECES
        dma = pltpu.SemaphoreType.DMA
        hbm = pl.BlockSpec(memory_space=pl.ANY)
        vmem = pl.BlockSpec(memory_space=pltpu.VMEM)
        n_w = len(W_SENDS)
        result = pl.pallas_call(
            functools.partial(moe_kernel, side),
            out_shape=pltpu.VMEM((rows, width), jnp.bfloat16),
            in_specs=[hbm, vmem, vmem, vmem, hbm, hbm, hbm],
            out_specs=vmem,
            scratch_shapes=[
                pltpu.VMEM((side, rows, width), jnp.bfloat16),
                pltpu.VMEM((group, rows), jnp.float32),
                pltpu.VMEM((side, num_q, rows), jnp.float32),
                pltpu.VMEM((num_q, rows), jnp.float32),
                pltpu.VMEM((2, rows, 2 * num_q), jnp.float32),
                pltpu.VMEM((side, PIECES, CORES, width, 2 * fp), jnp.bfloat16),
                pltpu.VMEM((side, PIECES, CORES, ff, dp), jnp.bfloat16),
                pltpu.VMEM((3 * num_q + num_q // 2, rows, ff), jnp.bfloat16),
                pltpu.VMEM((2, PIECES, rows, dp), jnp.float32),
                pltpu.VMEM((PIECES, rows, dp), jnp.float32),
                dma((3 * PIECES + 2,)), dma((2 * PIECES,)), dma((2 * PIECES,)),
                dma((n_w,)), dma((n_w,)), dma((n_w,)), dma((n_w,)),
                dma((6,)), dma((6,)), dma((4,)), dma((4,)),
                dma((3, PIECES, HALVES)), dma((3, PIECES, HALVES)),
                pltpu.SemaphoreType.REGULAR((2, PIECES, HALVES)),
            ],
            compiler_params=pltpu.CompilerParams(collective_id=0, has_side_effects=True, vmem_limit_bytes=67043328 - rows * width * 2),
        )(tokens, expert_ids.T, gate_wts.T, slot_ids.T, w_gate, w_up, w_down)
        return pl.pallas_call(
            place_kernel,
            out_shape=jax.ShapeDtypeStruct((rows, width), jnp.bfloat16),
            in_specs=[vmem],
            out_specs=hbm,
            scratch_shapes=[dma((1,))],
            compiler_params=pltpu.CompilerParams(vmem_limit_bytes=1 << 20),
        )(result)

    return jax.shard_map(per_device, mesh=mesh, in_specs=(row_spec, row_spec, row_spec, row_spec, expert_spec, expert_spec, expert_spec), out_specs=row_spec, check_vma=False)
```
